32 devices in a mesh: dp: 1 (over z), tp: 32 (over y, x, core).
Axes of the slice: x: 4, y: 4, z: 1, core: 2. Of those that a mesh axis runs over, the one named last changes fastest.
The devices are a block of a 4x4x8 slice.
Arguments:
- x: bfloat16 [192, 2048], P('dp')
- lengths: int32 [65], P('dp')
- attn_gain: bfloat16 [2, 2048], replicated
- w_q: bfloat16 [2, 2048, 2048], P(None, None, 'tp')
- w_k: bfloat16 [2, 2048, 2048], P(None, None, 'tp')
- w_v: bfloat16 [2, 2048, 2048], P(None, None, 'tp')
- w_o: bfloat16 [2, 2048, 2048], P(None, 'tp')
- mlp_gain: bfloat16 [2, 2048], replicated
- w_gate: bfloat16 [2, 2048, 8192], P(None, None, 'tp')
- w_up: bfloat16 [2, 2048, 8192], P(None, None, 'tp')
- w_down: bfloat16 [2, 8192, 2048], P(None, 'tp')
- k_cache: bfloat16 [2, 65, 32, 1024, 64], P(None, 'dp', 'tp')
- v_cache: bfloat16 [2, 65, 32, 1024, 64], P(None, 'dp', 'tp')
Outputs:
- output: bfloat16 [192, 2048], P('dp')
All inputs are finite; a program needn't handle non-finite values.
Results may differ from the reference program's by a relative error of at most 0.02.
Values are sent between devices in bfloat16 or wider.
A program may use at most 768 MiB of HBM per device.

```python
import jax
import jax.numpy as jnp
from jax import lax

D = 2048
HEADS = 32
KV_HEADS = 32
HEAD = 64
FF = 8192
BATCH = 64
CHUNK = 128
SEQ = 1024
LAYERS = 2

GROUP = HEADS // KV_HEADS
TOKENS = BATCH + CHUNK
ATTN_SCALE = HEAD ** -0.5
ROPE_BASE = 500000.0
EPSILON = 1e-5


def setup_inputs(seed: int = 0, part: int = 0) -> dict:
    root_key = jax.random.key(seed)
    shared_keys = jax.random.split(root_key, 9)
    part_keys = jax.random.split(jax.random.fold_in(root_key, part), 8)

    def gaussian(sub_key, arr_shape, factor):
        return jax.random.normal(sub_key, arr_shape, jnp.float32) * factor

    lengths = jax.random.randint(part_keys[1], (BATCH + 1,), 1, SEQ)
    longest = jax.random.randint(part_keys[2], (), 0, BATCH + 1)
    lengths = jnp.where(jnp.arange(BATCH + 1) == longest, SEQ - 1, lengths).astype(jnp.int32)
    pos_ramp = (jnp.arange(SEQ, dtype=jnp.float32) * (2.0 / SEQ) - 1.0)[:, None]
    cache_shape = (LAYERS, BATCH + 1, KV_HEADS, SEQ, HEAD)
    row_shape = (LAYERS, BATCH + 1, KV_HEADS, 1, HEAD)
    k_cache = gaussian(part_keys[3], cache_shape, 1.0) + pos_ramp * gaussian(part_keys[4], row_shape, 1.0)
    v_cache = gaussian(part_keys[5], row_shape, 1.0) + pos_ramp * gaussian(part_keys[6], row_shape, 1.0) + gaussian(part_keys[7], cache_shape, 0.5)
    return {
        'x': gaussian(part_keys[0], (TOKENS, D), 1.0).astype(jnp.bfloat16),
        'lengths': lengths,
        'attn_gain': jax.random.uniform(shared_keys[0], (LAYERS, D), jnp.float32, 0.5, 1.5).astype(jnp.bfloat16),
        'w_q': gaussian(shared_keys[1], (LAYERS, D, HEADS * HEAD), D ** -0.5).astype(jnp.bfloat16),
        'w_k': gaussian(shared_keys[2], (LAYERS, D, KV_HEADS * HEAD), D ** -0.5).astype(jnp.bfloat16),
        'w_v': gaussian(shared_keys[3], (LAYERS, D, KV_HEADS * HEAD), D ** -0.5).astype(jnp.bfloat16),
        'w_o': gaussian(shared_keys[4], (LAYERS, HEADS * HEAD, D), (HEADS * HEAD) ** -0.5).astype(jnp.bfloat16),
        'mlp_gain': jax.random.uniform(shared_keys[5], (LAYERS, D), jnp.float32, 0.5, 1.5).astype(jnp.bfloat16),
        'w_gate': gaussian(shared_keys[6], (LAYERS, D, FF), D ** -0.5).astype(jnp.bfloat16),
        'w_up': gaussian(shared_keys[7], (LAYERS, D, FF), D ** -0.5).astype(jnp.bfloat16),
        'w_down': gaussian(shared_keys[8], (LAYERS, FF, D), 1.5 * FF ** -0.5).astype(jnp.bfloat16),
        'k_cache': k_cache.astype(jnp.bfloat16),
        'v_cache': v_cache.astype(jnp.bfloat16),
    }


def rms_norm(x, norm_gain):
    x_f32 = x.astype(jnp.float32)
    inv_rms = lax.rsqrt(jnp.mean(x_f32 * x_f32, axis=-1, keepdims=True) + EPSILON)
    return (x_f32 * inv_rms * norm_gain.astype(jnp.float32)).astype(jnp.bfloat16)


def rope_tables(positions):
    freq_exps = jnp.arange(0, HEAD, 2, dtype=jnp.float32) / HEAD
    angles = positions.astype(jnp.float32)[:, None] * jnp.power(ROPE_BASE, -freq_exps)[None, :]
    return jnp.cos(angles)[:, None, :], jnp.sin(angles)[:, None, :]


def apply_rope(vectors, cos_tab, sin_tab):
    half_dim = HEAD // 2
    vec_f32 = vectors.astype(jnp.float32)
    first = vec_f32[..., :half_dim]
    second = vec_f32[..., half_dim:]
    return jnp.concatenate([first * cos_tab - second * sin_tab, second * cos_tab + first * sin_tab], axis=-1).astype(jnp.bfloat16)


def decode_row(row_args):
    q_row, k_row, v_row, kc_row, vc_row, length = row_args
    q_f32 = q_row.reshape(KV_HEADS, GROUP, HEAD).astype(jnp.float32)
    logits_cache = jnp.einsum('grd,gsd->grs', q_f32, kc_row.astype(jnp.float32)) * ATTN_SCALE
    logits_cache = jnp.where(jnp.arange(SEQ)[None, None, :] < length, logits_cache, -jnp.inf)
    logits_self = jnp.einsum('grd,gd->gr', q_f32, k_row.astype(jnp.float32))[:, :, None] * ATTN_SCALE
    prob_all = jax.nn.softmax(jnp.concatenate([logits_cache, logits_self], axis=-1), axis=-1)
    prob_all = prob_all.astype(jnp.bfloat16).astype(jnp.float32)
    result = jnp.einsum('grs,gsd->grd', prob_all[..., :SEQ], vc_row.astype(jnp.float32)) + prob_all[..., SEQ:] * v_row.astype(jnp.float32)[:, None, :]
    return result.astype(jnp.bfloat16).reshape(HEADS * HEAD)


def chunk_attention(q_chk, k_chk, v_chk, kc_row, vc_row, prefix_len):
    q_heads = q_chk.reshape(CHUNK, KV_HEADS, GROUP, HEAD).transpose(1, 0, 2, 3)
    k_heads = k_chk.transpose(1, 0, 2)
    v_heads = v_chk.transpose(1, 0, 2)
    cache_mask = jnp.arange(SEQ)[None, None, :] < prefix_len
    tok_ids = jnp.arange(CHUNK)
    causal_mask = (tok_ids[None, :] <= tok_ids[:, None])[:, None, :]

    def one_head(head_args):
        q_head, k_head, v_head, kc_head, vc_head = head_args
        q_f32 = q_head.astype(jnp.float32)
        logits_cache = jnp.einsum('crd,sd->crs', q_f32, kc_head.astype(jnp.float32)) * ATTN_SCALE
        logits_cache = jnp.where(cache_mask, logits_cache, -jnp.inf)
        logits_new = jnp.einsum('crd,jd->crj', q_f32, k_head.astype(jnp.float32)) * ATTN_SCALE
        logits_new = jnp.where(causal_mask, logits_new, -jnp.inf)
        prob_all = jax.nn.softmax(jnp.concatenate([logits_cache, logits_new], axis=-1), axis=-1)
        prob_all = prob_all.astype(jnp.bfloat16).astype(jnp.float32)
        result = jnp.einsum('crs,sd->crd', prob_all[..., :SEQ], vc_head.astype(jnp.float32)) + jnp.einsum('crj,jd->crd', prob_all[..., SEQ:], v_head.astype(jnp.float32))
        return result.astype(jnp.bfloat16)

    heads_out = lax.map(one_head, (q_heads, k_heads, v_heads, kc_row, vc_row))
    return heads_out.transpose(1, 0, 2, 3).reshape(CHUNK, HEADS * HEAD)


def decoder_layer(x, lengths, cos_tab, sin_tab, params):
    attn_gain, w_q, w_k, w_v, w_o, mlp_gain, w_gate, w_up, w_down, k_cache, v_cache = params
    normed = rms_norm(x, attn_gain)
    q_all = apply_rope(jnp.dot(normed, w_q, preferred_element_type=jnp.float32).astype(jnp.bfloat16).reshape(TOKENS, HEADS, HEAD), cos_tab, sin_tab)
    k_all = apply_rope(jnp.dot(normed, w_k, preferred_element_type=jnp.float32).astype(jnp.bfloat16).reshape(TOKENS, KV_HEADS, HEAD), cos_tab, sin_tab)
    v_all = jnp.dot(normed, w_v, preferred_element_type=jnp.float32).astype(jnp.bfloat16).reshape(TOKENS, KV_HEADS, HEAD)
    dec_out = lax.map(decode_row, (q_all[:BATCH], k_all[:BATCH], v_all[:BATCH], k_cache[:BATCH], v_cache[:BATCH], lengths[:BATCH]))
    chk_out = chunk_attention(q_all[BATCH:], k_all[BATCH:], v_all[BATCH:], k_cache[BATCH], v_cache[BATCH], lengths[BATCH])
    attended = jnp.concatenate([dec_out, chk_out], axis=0)
    hidden = (x.astype(jnp.float32) + jnp.dot(attended, w_o, preferred_element_type=jnp.float32)).astype(jnp.bfloat16)
    mlp_in = rms_norm(hidden, mlp_gain)
    gate_proj = jnp.dot(mlp_in, w_gate, preferred_element_type=jnp.float32)
    up_proj = jnp.dot(mlp_in, w_up, preferred_element_type=jnp.float32)
    activated = (jax.nn.silu(gate_proj) * up_proj).astype(jnp.bfloat16)
    down_proj = jnp.dot(activated, w_down, preferred_element_type=jnp.float32)
    return (hidden.astype(jnp.float32) + down_proj).astype(jnp.bfloat16)


def reference(x, lengths, attn_gain, w_q, w_k, w_v, w_o, mlp_gain, w_gate, w_up, w_down, k_cache, v_cache):
    positions = jnp.concatenate([lengths[:BATCH], lengths[BATCH] + jnp.arange(CHUNK, dtype=jnp.int32)])
    cos_tab, sin_tab = rope_tables(positions)

    def layer_step(hidden, params):
        return decoder_layer(hidden, lengths, cos_tab, sin_tab, params), None

    result, unused = lax.scan(layer_step, x, (attn_gain, w_q, w_k, w_v, w_o, mlp_gain, w_gate, w_up, w_down, k_cache, v_cache))
    return result
```

```python
import functools

import jax
import jax.numpy as jnp
from jax import lax
from jax.experimental import pallas as pl
from jax.experimental.pallas import tpu as pltpu
from jax.sharding import PartitionSpec as P

ROPE_BASE = 500000.0
EPSILON = 1e-5
MESH = pl.DeviceIdType.MESH
LANES = 128
BLOCK = 16
F32 = jnp.float32
BF16 = jnp.bfloat16


def rope_tables(positions, head_dim):
    freq_exps = jnp.arange(0, head_dim, 2, dtype=F32) / head_dim
    angles = positions.astype(F32)[:, None] * jnp.power(ROPE_BASE, -freq_exps)[None, :]
    cos, sin = jnp.cos(angles), jnp.sin(angles)
    return jnp.concatenate([cos, cos, cos, cos], axis=1), jnp.concatenate([-sin, sin, -sin, sin], axis=1)


def tables(lengths, tok, head_dim, gains):
    dec = lengths.shape[0] - 1
    positions = jnp.concatenate([lengths[:dec], lengths[dec] + jnp.arange(tok - dec, dtype=jnp.int32)])
    cos_tab, sin_tab = rope_tables(positions, head_dim)
    len_tab = jnp.broadcast_to(jnp.concatenate([lengths[:dec], jnp.broadcast_to(lengths[dec:], (8,))])[:, None], (dec + 8, LANES))
    return len_tab, cos_tab, sin_tab, gains.astype(F32).reshape(-1, LANES)


def nt_dot(a, b):
    return lax.dot_general(a, b, (((1,), (1,)), ((), ())), preferred_element_type=F32)


def layers_kernel(dims, x_hbm, len_ref, cos_ref, sin_ref, gain_ref, wq_hbm, wk_hbm, wv_hbm, wo_hbm, wg_hbm, wu_hbm, wd_hbm, kc_hbm, vc_hbm, out_hbm,
                  hbuf, part, pair_in, mine, rs_in, normed, qkv, qbd, logits, probs, attended, act,
                  wqkv, wo, wg, wu, wd, kc, vc,
                  x_sem, w_sem, out_sem, pair_send, pair_recv, rs_send, rs_recv, ag_send, ag_recv, fwd_send, fwd_recv):
    n, layers, tok, width, dec, seq, hd, ff = dims
    chips = n // 2
    side = int(round(chips ** 0.5))
    half = tok // 2
    chunk = tok - dec
    ncol = width // LANES
    me = lax.axis_index("tp")
    core = lax.rem(me, 2)
    chip = me // 2
    my_y, my_x = chip // side, lax.rem(chip, side)
    partner = chip * 2 + (1 - core)
    my_rows = pl.ds(pl.multiple_of(core * half, half), half)
    other_rows = pl.ds(pl.multiple_of((1 - core) * half, half), half)

    def peer_chip(step):
        return lax.rem(my_y + step // side, side) * side + lax.rem(my_x + lax.rem(step, side), side)

    barrier = pltpu.get_barrier_semaphore()
    pl.semaphore_signal(barrier, inc=1, device_id={"tp": partner}, device_id_type=MESH)

    def greet(step, carry):
        pl.semaphore_signal(barrier, inc=1, device_id={"tp": peer_chip(step) * 2 + core}, device_id_type=MESH)
        return carry

    lax.fori_loop(1, chips, greet, 0)

    def x_copy(c):
        return pltpu.make_async_copy(x_hbm.at[:, pl.ds(c * LANES, LANES)], hbuf.at[c], x_sem.at[c])

    def load(l, name):
        i, src, dst = {
            "q": (0, wq_hbm, wqkv.at[l, pl.ds(0, hd)]),
            "k": (1, wk_hbm, wqkv.at[l, pl.ds(hd, hd)]),
            "v": (2, wv_hbm, wqkv.at[l, pl.ds(2 * hd, hd)]),
            "o": (3, wo_hbm, wo.at[l]),
            "gate": (4, wg_hbm, wg.at[l]),
            "up": (5, wu_hbm, wu.at[l]),
            "down": (6, wd_hbm, wd.at[l]),
            "keys": (7, kc_hbm, kc.at[l]),
            "values": (8, vc_hbm, vc.at[l]),
        }[name]
        return pltpu.make_async_copy(src.at[l], dst, w_sem.at[l, i])

    def load_all(l):
        for name in ("q", "k", "v", "keys", "values", "o", "gate", "up", "down"):
            load(l, name).start()

    for c in range(ncol):
        x_copy(c).start()
    load_all(0)
    for c in range(ncol):
        x_copy(c).wait()

    def norm(gain_row):
        def square(c, acc):
            h = hbuf[c].astype(F32)
            return acc + h * h

        total = lax.fori_loop(0, ncol, square, jnp.zeros((tok, LANES), F32))
        inv = lax.rsqrt(jnp.sum(total, axis=1, keepdims=True) / width + EPSILON)

        def scale(c, carry):
            gain = gain_ref[pl.ds(gain_row * ncol + c, 1), :]
            normed[:, pl.ds(pl.multiple_of(c * LANES, LANES), LANES)] = (hbuf[c].astype(F32) * inv * gain).astype(BF16)
            return carry

        lax.fori_loop(0, ncol, scale, 0)

    def attention(l):
        for name in ("q", "k", "v"):
            load(l, name).wait()
        proj = nt_dot(normed[...], wqkv[l]).astype(BF16)
        lane = lax.broadcasted_iota(jnp.int32, (tok, LANES), 1)
        qk = proj[:, :2 * hd].astype(F32)
        turned = jnp.where(lax.rem(lane, hd) < hd // 2, pltpu.roll(qk, LANES - hd // 2, 1), pltpu.roll(qk, hd // 2, 1))
        qk = (qk * cos_ref[...] + turned * sin_ref[...]).astype(BF16).astype(F32)
        qkv[:, :2 * hd] = qk.astype(BF16)
        qkv[:, 2 * hd:3 * hd] = proj[:, 2 * hd:]
        qk_dec = qk[:dec]
        q_twice = jnp.where(lane[:dec] < hd, qk_dec, pltpu.roll(qk_dec, hd, 1))
        row = lax.rem(lax.broadcasted_iota(jnp.int32, (dec, LANES), 0), BLOCK)
        for j in range(BLOCK * hd // LANES):
            keep = row == 2 * j + lane[:dec] // hd
            qbd[:, j * LANES:(j + 1) * LANES] = jnp.where(keep, q_twice, 0.0).astype(BF16)
        k_twice = jnp.where(lane[:dec] < hd, pltpu.roll(qk_dec, hd, 1), qk_dec)
        scale = hd ** -0.5
        self_logit = jnp.sum(jnp.where(lane[:dec] < hd, q_twice * k_twice, 0.0), axis=1, keepdims=True) * scale
        load(l, "keys").wait()
        span = BLOCK * hd

        def dec_logits(g, carry):
            rows = pl.ds(pl.multiple_of(g * BLOCK, BLOCK), BLOCK)
            keys = kc[l, pl.ds(pl.multiple_of(g * span, span), span), :]
            logits[rows, :] = jnp.dot(qbd[rows, :], keys, preferred_element_type=F32)
            return carry

        lax.fori_loop(0, dec // BLOCK, dec_logits, 0)
        lens = len_ref[0:dec, 0:1]
        pos = lax.broadcasted_iota(jnp.int32, (dec, seq), 1)
        lg = jnp.where(pos < lens, logits[0:dec, :] * scale, -jnp.inf)
        top = jnp.maximum(jnp.max(lg, axis=1, keepdims=True), self_logit)
        ex = jnp.exp(lg - top)
        ex_self = jnp.exp(self_logit - top)
        inv = 1.0 / (jnp.sum(ex, axis=1, keepdims=True) + ex_self)
        probs[0:dec, :] = (ex * inv).astype(BF16)
        p_self = (ex_self * inv).astype(BF16).astype(F32)
        q_chk = qkv[dec:, 0:hd]
        lg = jnp.dot(q_chk, kc[l, dec * hd:(dec + 1) * hd, :], preferred_element_type=F32) * scale
        lg_new = nt_dot(q_chk, qkv[dec:, hd:2 * hd]) * scale
        pos = lax.broadcasted_iota(jnp.int32, (chunk, seq), 1)
        lg = jnp.where(pos < len_ref[dec:dec + 1, 0:1], lg, -jnp.inf)
        tok_r = lax.broadcasted_iota(jnp.int32, (chunk, chunk), 0)
        tok_c = lax.broadcasted_iota(jnp.int32, (chunk, chunk), 1)
        lg_new = jnp.where(tok_c <= tok_r, lg_new, -jnp.inf)
        top = jnp.maximum(jnp.max(lg, axis=1, keepdims=True), jnp.max(lg_new, axis=1, keepdims=True))
        ex, ex_new = jnp.exp(lg - top), jnp.exp(lg_new - top)
        inv = 1.0 / (jnp.sum(ex, axis=1, keepdims=True) + jnp.sum(ex_new, axis=1, keepdims=True))
        probs[dec:, :] = (ex * inv).astype(BF16)
        p_new = (ex_new * inv).astype(BF16)
        load(l, "values").wait()
        lane_b = lax.broadcasted_iota(jnp.int32, (BLOCK, LANES), 1)
        row_b = lax.broadcasted_iota(jnp.int32, (BLOCK, LANES), 0)

        def dec_values(g, carry):
            rows = pl.ds(pl.multiple_of(g * BLOCK, BLOCK), BLOCK)
            full = nt_dot(probs[rows, :], vc[l, pl.ds(pl.multiple_of(g * span, span), span), :])
            acc = jnp.zeros((BLOCK, LANES), F32)
            for j in range(BLOCK * hd // LANES):
                acc += jnp.where(row_b == 2 * j + lane_b // hd, full[:, j * LANES:(j + 1) * LANES], 0.0)
            logits[rows, 0:LANES] = acc + pltpu.roll(acc, hd, 1)
            return carry

        lax.fori_loop(0, dec // BLOCK, dec_values, 0)
        attended[0:dec, :] = (logits[0:dec, 0:hd] + p_self * qkv[0:dec, 2 * hd:3 * hd].astype(F32)).astype(BF16)
        out = nt_dot(probs[dec:, :], vc[l, dec * hd:(dec + 1) * hd, :])
        out += jnp.dot(p_new, qkv[dec:, 2 * hd:3 * hd], preferred_element_type=F32)
        attended[dec:, :] = out.astype(BF16)
        load(l, "o").wait()
        project_out(attended, wo.at[l])

    def project_out(lhs_ref, w_ref):
        lhs = lhs_ref[...]
        for c in range(0, ncol, 4):
            out = jnp.dot(lhs, w_ref[:, c * LANES:(c + 4) * LANES], preferred_element_type=F32).astype(BF16)
            for j in range(4):
                part[c + j] = out[:, j * LANES:(j + 1) * LANES]

    def mlp(l):
        for name in ("gate", "up", "down"):
            load(l, name).wait()
        a = normed[...]
        gate = jnp.dot(a, wg[l], preferred_element_type=F32)
        up = jnp.dot(a, wu[l], preferred_element_type=F32)
        act[...] = (gate * lax.logistic(gate) * up).astype(BF16)
        project_out(act, wd.at[l])

    def remote(src, dst, send, recv, dev):
        return pltpu.make_async_remote_copy(src_ref=src, dst_ref=dst, send_sem=send, recv_sem=recv, device_id={"tp": dev}, device_id_type=MESH)

    def reduce_and_spread():
        pair = remote(part.at[:, other_rows], pair_in, pair_send.at[0], pair_recv.at[0], partner)
        pair.start()
        pair.wait()

        def combine(c):
            return part[c, my_rows, :].astype(F32) + pair_in[c].astype(F32)

        def scatter(step, carry):
            to = peer_chip(step)
            mine[to] = combine(to).astype(BF16)
            remote(mine.at[to], rs_in.at[chip], rs_send.at[0], rs_recv.at[0], to * 2 + core).start()
            return carry

        lax.fori_loop(1, chips, scatter, 0)
        acc = combine(chip) + hbuf[chip, my_rows, :].astype(F32)
        rest = mine.at[pl.ds(0, chips - 1)]
        whole = remote(rest, rs_in.at[pl.ds(0, chips - 1)], rs_send.at[0], rs_recv.at[0], partner)
        whole.wait_recv()

        def gather_sum(step, acc):
            return acc + rs_in[peer_chip(step)].astype(F32)

        acc = lax.fori_loop(1, chips, gather_sum, acc)
        hbuf[chip, my_rows, :] = acc.astype(BF16)
        own = hbuf.at[chip, my_rows]

        def spread(step, carry):
            remote(own, own, ag_send.at[0], ag_recv.at[chip], peer_chip(step) * 2 + core).start()
            return carry

        lax.fori_loop(1, chips, spread, 0)
        remote(own, own, fwd_send.at[0], fwd_recv.at[0], partner).start()

        def forward(step, carry):
            at = peer_chip(step)
            block = hbuf.at[at, my_rows]
            remote(block, block, ag_send.at[0], ag_recv.at[at], partner).wait_recv()
            remote(block, block, fwd_send.at[0], fwd_recv.at[0], partner).start()
            return carry

        lax.fori_loop(1, chips, forward, 0)
        whole.wait_send()
        remote(rest, rest, ag_send.at[0], rs_recv.at[0], partner).wait_send()
        remote(hbuf.at[:, my_rows], hbuf.at[:, other_rows], fwd_send.at[0], fwd_recv.at[0], partner).wait()

    for l in range(layers):
        norm(2 * l)
        attention(l)
        if l == 0:
            for later in range(1, layers):
                load_all(later)
            pl.semaphore_wait(barrier, chips)
        reduce_and_spread()
        norm(2 * l + 1)
        mlp(l)
        reduce_and_spread()

    def out_copy(c):
        return pltpu.make_async_copy(hbuf.at[c], out_hbm.at[:, pl.ds(c * LANES, LANES)], out_sem.at[c])

    for c in range(ncol):
        out_copy(c).start()
    for c in range(ncol):
        out_copy(c).wait()


def solution(mesh):
    col_spec = P(None, None, "tp")
    row_spec = P(None, "tp", None)
    cache_spec = P(None, "dp", "tp", None, None)
    in_specs = (P("dp", None), P("dp"), P(), col_spec, col_spec, col_spec, row_spec, P(), col_spec, col_spec, row_spec, cache_spec, cache_spec)
    n = mesh.shape["tp"]

    def body(x, lengths, attn_gain, w_q, w_k, w_v, w_o, mlp_gain, w_gate, w_up, w_down, k_cache, v_cache):
        tok, width = x.shape
        layers, rows, _, seq, hd = k_cache.shape
        dec, ff, chips = rows - 1, w_gate.shape[-1], n // 2
        half, ncol = tok // 2, width // LANES
        gains = jnp.stack([attn_gain, mlp_gain], axis=1)
        small = tables(lengths, tok, hd, gains)

        def flat(cache):
            return jnp.swapaxes(cache, 3, 4).reshape(layers, rows * hd, seq)

        def turned(w):
            return jnp.swapaxes(w, 1, 2)

        dma = pltpu.SemaphoreType.DMA
        vmem, hbm = pl.BlockSpec(memory_space=pltpu.VMEM), pl.BlockSpec(memory_space=pl.ANY)
        return pl.pallas_call(
            functools.partial(layers_kernel, (n, layers, tok, width, dec, seq, hd, ff)),
            out_shape=jax.ShapeDtypeStruct((tok, width), BF16),
            in_specs=[hbm] + [vmem] * 4 + [hbm] * 9,
            out_specs=hbm,
            scratch_shapes=[
                pltpu.VMEM((ncol, tok, LANES), BF16),
                pltpu.VMEM((ncol, tok, LANES), BF16),
                pltpu.VMEM((ncol, half, LANES), BF16),
                pltpu.VMEM((ncol, half, LANES), BF16),
                pltpu.VMEM((ncol, half, LANES), BF16),
                pltpu.VMEM((tok, width), BF16),
                pltpu.VMEM((tok, 3 * hd), BF16),
                pltpu.VMEM((dec, BLOCK * hd), BF16),
                pltpu.VMEM((dec, seq), F32),
                pltpu.VMEM((tok, seq), BF16),
                pltpu.VMEM((tok, hd), BF16),
                pltpu.VMEM((tok, ff), BF16),
                pltpu.VMEM((layers, 3 * hd, width), BF16),
                pltpu.VMEM((layers, hd, width), BF16),
                pltpu.VMEM((layers, width, ff), BF16),
                pltpu.VMEM((layers, width, ff), BF16),
                pltpu.VMEM((layers, ff, width), BF16),
                pltpu.VMEM((layers, rows * hd, seq), BF16),
                pltpu.VMEM((layers, rows * hd, seq), BF16),
                dma((ncol,)),
                dma((layers, 9)),
                dma((ncol,)),
                dma((1,)), dma((1,)), dma((1,)), dma((1,)), dma((1,)), dma((chips,)), dma((1,)), dma((1,)),
            ],
            compiler_params=pltpu.CompilerParams(collective_id=0, has_side_effects=True, vmem_limit_bytes=60 * 2**20),
        )(x, *small, turned(w_q), turned(w_k), turned(w_v), w_o, w_gate, w_up, w_down, flat(k_cache), flat(v_cache))

    return jax.shard_map(body, mesh=mesh, in_specs=in_specs, out_specs=P("dp", None), check_vma=False)
```

```python
import functools

import jax
import jax.numpy as jnp
from jax import lax
from jax.experimental import pallas as pl
from jax.experimental.pallas import tpu as pltpu
from jax.sharding import PartitionSpec as P

ROPE_BASE = 500000.0
EPSILON = 1e-5
MESH = pl.DeviceIdType.MESH
LANES = 128
SUBLANES = 8
BLOCK = 16
F32 = jnp.float32
BF16 = jnp.bfloat16


def nt_dot(a, b):
    return lax.dot_general(a, b, (((1,), (1,)), ((), ())), preferred_element_type=F32)


def layers_kernel(dims, len_ref, again_ref, mgain_ref, x_hbm, wq_hbm, wk_hbm, wv_hbm, wo_hbm, wg_hbm, wu_hbm, wd_hbm, kc_hbm, vc_hbm, out_ref,
                  hbuf, part, pair_in, mine, rs_in, normed, qkv, qbd, logits, probs, attended, act, cos_ref, sin_ref, len_col, gains,
                  wqkv, wo, wg, wu, wd, kc, vc,
                  x_sem, w_sem, pair_send, pair_recv, rs_send, rs_recv, ag_send, ag_recv, fwd_send, fwd_recv):
    n, layers, tok, width, dec, seq, hd, ff = dims
    chips = n // 2
    side = int(round(chips ** 0.5))
    chunk = tok - dec
    ncol = width // LANES
    ngrp = ncol // 2
    me = lax.axis_index("tp")
    core = lax.rem(me, 2)
    chip = me // 2
    my_y, my_x = chip // side, lax.rem(chip, side)
    partner = chip * 2 + (1 - core)
    my_base, other_base = core * ngrp, (1 - core) * ngrp
    streams = ((0, dec), (dec, chunk))
    DEC, PRE = 0, 1

    def peer_chip(step):
        return lax.rem(my_y + step // side, side) * side + lax.rem(my_x + lax.rem(step, side), side)

    barrier = pltpu.get_barrier_semaphore()
    pl.semaphore_signal(barrier, inc=1, device_id={"tp": partner}, device_id_type=MESH)

    def greet(step, carry):
        pl.semaphore_signal(barrier, inc=1, device_id={"tp": peer_chip(step) * 2 + core}, device_id_type=MESH)
        return carry

    lax.fori_loop(1, chips, greet, 0)

    def x_copy(c):
        return pltpu.make_async_copy(x_hbm.at[:, pl.ds(c * LANES, LANES)], hbuf.at[c], x_sem.at[c])

    def load(l, name):
        if name == "pre_keys":
            return pltpu.make_async_copy(kc_hbm.at[l, pl.ds(dec * hd, hd)], kc.at[l, pl.ds(dec * hd, hd)], w_sem.at[l, 9])
        if name == "pre_values":
            return pltpu.make_async_copy(vc_hbm.at[l, pl.ds(dec * hd, hd)], vc.at[l, pl.ds(dec * hd, hd)], w_sem.at[l, 10])
        i, src, dst = {
            "q": (0, wq_hbm.at[l], wqkv.at[l, pl.ds(0, hd)]),
            "k": (1, wk_hbm.at[l], wqkv.at[l, pl.ds(hd, hd)]),
            "v": (2, wv_hbm.at[l], wqkv.at[l, pl.ds(2 * hd, hd)]),
            "o": (3, wo_hbm.at[l], wo.at[l]),
            "gate": (4, wg_hbm.at[l], wg.at[l]),
            "up": (5, wu_hbm.at[l], wu.at[l]),
            "down": (6, wd_hbm.at[l], wd.at[l]),
            "keys": (7, kc_hbm.at[l, pl.ds(0, dec * hd)], kc.at[l, pl.ds(0, dec * hd)]),
            "values": (8, vc_hbm.at[l, pl.ds(0, dec * hd)], vc.at[l, pl.ds(0, dec * hd)]),
        }[name]
        return pltpu.make_async_copy(src, dst, w_sem.at[l, i])

    def load_all(l):
        for name in ("q", "k", "v", "pre_keys", "pre_values", "o", "keys", "values", "gate", "up", "down"):
            load(l, name).start()

    for c in range(ncol):
        x_copy(c).start()
    load_all(0)

    row8 = lax.broadcasted_iota(jnp.int32, (SUBLANES, LANES), 0)
    for b in range(dec // SUBLANES):
        col = jnp.zeros((SUBLANES, LANES), jnp.int32)
        for i in range(SUBLANES):
            col = jnp.where(row8 == i, len_ref[b * SUBLANES + i], col)
        len_col[b * SUBLANES:(b + 1) * SUBLANES, :] = col
    prefix = len_ref[dec]
    lane_f = lax.broadcasted_iota(jnp.int32, (1, LANES), 1)
    freq_exps = (2 * lax.rem(lane_f, hd // 2)).astype(F32) / hd
    freqs = jnp.exp(-freq_exps * jnp.log(jnp.full((1, LANES), ROPE_BASE, F32)))
    sign = jnp.where(lax.rem(lane_f, hd) < hd // 2, -1.0, 1.0)
    pos = jnp.concatenate([len_col[...], prefix + lax.broadcasted_iota(jnp.int32, (chunk, LANES), 0)], axis=0)
    angles = pos.astype(F32) * freqs
    cos_ref[...] = jnp.cos(angles)
    sin_ref[...] = jnp.sin(angles) * sign
    gains[0:layers, :] = again_ref[...].astype(F32)
    gains[layers:, :] = mgain_ref[...].astype(F32)

    for c in range(ncol):
        x_copy(c).wait()

    def norm(s, gain_row):
        r0, rows = streams[s]
        total = jnp.zeros((rows, LANES), F32)
        for c in range(ncol):
            h = hbuf[c, r0:r0 + rows, :].astype(F32)
            total += h * h
        inv = lax.rsqrt(jnp.sum(total, axis=1, keepdims=True) / width + EPSILON)
        for c in range(ncol):
            gain = gains[gain_row:gain_row + 1, c * LANES:(c + 1) * LANES]
            normed[r0:r0 + rows, c * LANES:(c + 1) * LANES] = (hbuf[c, r0:r0 + rows, :].astype(F32) * inv * gain).astype(BF16)

    def project_qkv(s, l):
        r0, rows = streams[s]
        proj = nt_dot(normed[r0:r0 + rows, :], wqkv[l]).astype(BF16)
        lane = lax.broadcasted_iota(jnp.int32, (rows, LANES), 1)
        qk = proj[:, :2 * hd].astype(F32)
        turned = jnp.where(lax.rem(lane, hd) < hd // 2, pltpu.roll(qk, LANES - hd // 2, 1), pltpu.roll(qk, hd // 2, 1))
        qk = (qk * cos_ref[r0:r0 + rows, :] + turned * sin_ref[r0:r0 + rows, :]).astype(BF16)
        qkv[r0:r0 + rows, :2 * hd] = qk
        qkv[r0:r0 + rows, 2 * hd:3 * hd] = proj[:, 2 * hd:]

    scale = hd ** -0.5

    def decode_attention(l):
        lane = lax.broadcasted_iota(jnp.int32, (dec, LANES), 1)
        qk = qkv[0:dec, :2 * hd].astype(F32)
        swapped = pltpu.roll(qk, hd, 1)
        q_twice = jnp.where(lane < hd, qk, swapped)
        k_twice = jnp.where(lane < hd, swapped, qk)
        row = lax.rem(lax.broadcasted_iota(jnp.int32, (dec, LANES), 0), BLOCK)
        for j in range(BLOCK * hd // LANES):
            qbd[:, j * LANES:(j + 1) * LANES] = jnp.where(row == 2 * j + lane // hd, q_twice, 0.0).astype(BF16)
        self_logit = jnp.sum(jnp.where(lane < hd, q_twice * k_twice, 0.0), axis=1, keepdims=True) * scale
        span = BLOCK * hd

        def dec_logits(g, carry):
            rows = pl.ds(pl.multiple_of(g * BLOCK, BLOCK), BLOCK)
            keys = kc[l, pl.ds(pl.multiple_of(g * span, span), span), :]
            logits[rows, :] = jnp.dot(qbd[rows, :], keys, preferred_element_type=F32)
            return carry

        lax.fori_loop(0, dec // BLOCK, dec_logits, 0)
        pos = lax.broadcasted_iota(jnp.int32, (dec, seq), 1)
        lg = jnp.where(pos < len_col[:, 0:1], logits[0:dec, :] * scale, -jnp.inf)
        top = jnp.maximum(jnp.max(lg, axis=1, keepdims=True), self_logit)
        ex = jnp.exp(lg - top)
        ex_self = jnp.exp(self_logit - top)
        inv = 1.0 / (jnp.sum(ex, axis=1, keepdims=True) + ex_self)
        probs[0:dec, :] = (ex * inv).astype(BF16)
        p_self = (ex_self * inv).astype(BF16).astype(F32)
        lane_b = lax.broadcasted_iota(jnp.int32, (BLOCK, LANES), 1)
        row_b = lax.broadcasted_iota(jnp.int32, (BLOCK, LANES), 0)

        def dec_values(g, carry):
            rows = pl.ds(pl.multiple_of(g * BLOCK, BLOCK), BLOCK)
            full = nt_dot(probs[rows, :], vc[l, pl.ds(pl.multiple_of(g * span, span), span), :])
            acc = jnp.zeros((BLOCK, LANES), F32)
            for j in range(BLOCK * hd // LANES):
                acc += jnp.where(row_b == 2 * j + lane_b // hd, full[:, j * LANES:(j + 1) * LANES], 0.0)
            logits[rows, 0:LANES] = acc + pltpu.roll(acc, hd, 1)
            return carry

        lax.fori_loop(0, dec // BLOCK, dec_values, 0)
        attended[0:dec, :] = (logits[0:dec, 0:hd] + p_self * qkv[0:dec, 2 * hd:3 * hd].astype(F32)).astype(BF16)

    def prefill_attention(l):
        q_chk = qkv[dec:, 0:hd]
        lg = jnp.dot(q_chk, kc[l, dec * hd:(dec + 1) * hd, :], preferred_element_type=F32) * scale
        lg_new = nt_dot(q_chk, qkv[dec:, hd:2 * hd]) * scale
        pos = lax.broadcasted_iota(jnp.int32, (chunk, seq), 1)
        lg = jnp.where(pos < prefix, lg, -jnp.inf)
        tok_r = lax.broadcasted_iota(jnp.int32, (chunk, chunk), 0)
        tok_c = lax.broadcasted_iota(jnp.int32, (chunk, chunk), 1)
        lg_new = jnp.where(tok_c <= tok_r, lg_new, -jnp.inf)
        top = jnp.maximum(jnp.max(lg, axis=1, keepdims=True), jnp.max(lg_new, axis=1, keepdims=True))
        ex, ex_new = jnp.exp(lg - top), jnp.exp(lg_new - top)
        inv = 1.0 / (jnp.sum(ex, axis=1, keepdims=True) + jnp.sum(ex_new, axis=1, keepdims=True))
        p_old = (ex * inv).astype(BF16)
        p_new = (ex_new * inv).astype(BF16)
        out = nt_dot(p_old, vc[l, dec * hd:(dec + 1) * hd, :])
        out += jnp.dot(p_new, qkv[dec:, 2 * hd:3 * hd], preferred_element_type=F32)
        attended[dec:, :] = out.astype(BF16)

    def remote(src, dst, send, recv, dev):
        return pltpu.make_async_remote_copy(src_ref=src, dst_ref=dst, send_sem=send, recv_sem=recv, device_id={"tp": dev}, device_id_type=MESH)

    def pair_copy(s):
        r0, rows = streams[s]
        return remote(part.at[pl.ds(other_base, ngrp), pl.ds(r0, rows)], pair_in.at[:, pl.ds(r0, rows)], pair_send.at[s], pair_recv.at[s], partner)

    def project_out(s, lhs_ref, w_ref):
        r0, rows = streams[s]
        lhs = lhs_ref[r0:r0 + rows, :]
        step = min(4, ngrp)
        for base in (other_base, my_base):
            for c in range(0, ngrp, step):
                at = pl.multiple_of((base + c) * LANES, LANES)
                out = jnp.dot(lhs, w_ref[:, pl.ds(at, step * LANES)], preferred_element_type=F32).astype(BF16)
                for j in range(step):
                    part[base + c + j, r0:r0 + rows, :] = out[:, j * LANES:(j + 1) * LANES]
            if base is other_base:
                pair_copy(s).start()

    def block_at(s, c):
        r0, rows = streams[s]
        half = rows // 2
        return lax.rem(c, ngrp), pl.ds(pl.multiple_of(r0 + (c // ngrp) * half, half), half)

    def own_rows(s):
        r0, rows = streams[s]
        return pl.ds(r0 // 2, rows // 2)

    def start_compute(s, phase):
        l = phase // 2
        r0, rows = streams[s]
        norm(s, l + layers * (phase % 2))
        if phase % 2 == 0:
            if s == PRE:
                for name in ("q", "k", "v"):
                    load(l, name).wait()
            project_qkv(s, l)
        else:
            if s == PRE:
                load(l, "gate").wait()
                load(l, "up").wait()
            a = normed[r0:r0 + rows, :]
            gate = jnp.dot(a, wg[l], preferred_element_type=F32)
            up = jnp.dot(a, wu[l], preferred_element_type=F32)
            act[r0:r0 + rows, :] = (gate * lax.logistic(gate) * up).astype(BF16)

    def end_compute(s, phase):
        l = phase // 2
        if phase % 2 == 0:
            if s == PRE:
                load(l, "pre_keys").wait()
                load(l, "pre_values").wait()
                prefill_attention(l)
                load(l, "o").wait()
            else:
                load(l, "keys").wait()
                load(l, "values").wait()
                decode_attention(l)
            if phase == 0 and s == PRE:
                pl.semaphore_wait(barrier, chips)
            project_out(s, attended, wo.at[l])
        else:
            if s == PRE:
                load(l, "down").wait()
            project_out(s, act, wd.at[l])

    def combine(s, c):
        group, rows = block_at(s, c)
        return part[my_base + group, rows, :].astype(F32) + pair_in[group, rows, :].astype(F32)

    def scatter(s):
        pair_copy(s).wait()
        slot = own_rows(s)

        def send(step, carry):
            to = peer_chip(step)
            mine[to, slot, :] = combine(s, to).astype(BF16)
            remote(mine.at[to, slot], rs_in.at[chip, slot], rs_send.at[s], rs_recv.at[s], to * 2 + core).start()
            return carry

        lax.fori_loop(1, chips, send, 0)

    def scattered(s):
        blocks = pl.ds(0, chips - 1)
        return remote(mine.at[blocks, own_rows(s)], rs_in.at[blocks, own_rows(s)], rs_send.at[s], rs_recv.at[s], partner)

    def spread(s):
        group, rows = block_at(s, chip)
        own = hbuf.at[my_base + group, rows]
        acc = combine(s, chip) + hbuf[my_base + group, rows, :].astype(F32)
        scattered(s).wait_recv()

        def add(step, acc):
            return acc + rs_in[peer_chip(step), own_rows(s), :].astype(F32)

        hbuf[my_base + group, rows, :] = lax.fori_loop(1, chips, add, acc).astype(BF16)

        def send(step, carry):
            remote(own, own, ag_send.at[s], ag_recv.at[s, chip], peer_chip(step) * 2 + core).start()
            return carry

        lax.fori_loop(1, chips, send, 0)
        remote(own, own, fwd_send.at[s], fwd_recv.at[s], partner).start()

    def forward(s):
        def hand_on(step, carry):
            at = peer_chip(step)
            group, rows = block_at(s, at)
            block = hbuf.at[my_base + group, rows]
            remote(block, block, ag_send.at[s], ag_recv.at[s, at], partner).wait_recv()
            remote(block, block, fwd_send.at[s], fwd_recv.at[s], partner).start()
            return carry

        lax.fori_loop(1, chips, hand_on, 0)

    def finish(s):
        r0, rows = streams[s]
        blocks = pl.ds(0, chips - 1)
        scattered(s).wait_send()
        remote(mine.at[blocks, own_rows(s)], rs_in.at[blocks, own_rows(s)], ag_send.at[s], rs_recv.at[s], partner).wait_send()
        remote(hbuf.at[pl.ds(my_base, ngrp), pl.ds(r0, rows)], hbuf.at[pl.ds(other_base, ngrp), pl.ds(r0, rows)], fwd_send.at[s], fwd_recv.at[s], partner).wait()

    phases = 2 * layers
    start_compute(PRE, 0)
    end_compute(PRE, 0)
    for phase in range(phases):
        if phase > 0:
            forward(DEC)
            scatter(PRE)
            finish(DEC)
            start_compute(DEC, phase)
        else:
            start_compute(DEC, phase)
            scatter(PRE)
            for later in range(1, layers):
                load_all(later)
        end_compute(DEC, phase)
        scatter(DEC)
        spread(PRE)
        spread(DEC)
        forward(PRE)
        finish(PRE)
        if phase + 1 < phases:
            start_compute(PRE, phase + 1)
            end_compute(PRE, phase + 1)
    r0, rows = streams[PRE]
    for c in range(ncol):
        out_ref[r0:r0 + rows, c * LANES:(c + 1) * LANES] = hbuf[c, r0:r0 + rows, :]
    forward(DEC)
    finish(DEC)
    r0, rows = streams[DEC]
    for c in range(ncol):
        out_ref[r0:r0 + rows, c * LANES:(c + 1) * LANES] = hbuf[c, r0:r0 + rows, :]


def solution(mesh):
    col_spec = P(None, None, "tp")
    row_spec = P(None, "tp", None)
    cache_spec = P(None, "dp", "tp", None, None)
    in_specs = (P("dp", None), P("dp"), P(), col_spec, col_spec, col_spec, row_spec, P(), col_spec, col_spec, row_spec, cache_spec, cache_spec)
    n = mesh.shape["tp"]

    def body(x, lengths, attn_gain, w_q, w_k, w_v, w_o, mlp_gain, w_gate, w_up, w_down, k_cache, v_cache):
        tok, width = x.shape
        layers, rows, _, seq, hd = k_cache.shape
        dec, ff, chips = rows - 1, w_gate.shape[-1], n // 2
        half, ncol = tok // 2, width // LANES

        def flat(cache):
            return jnp.swapaxes(cache, 3, 4).reshape(layers, rows * hd, seq)

        def turned(w):
            return jnp.swapaxes(w, 1, 2)

        dma = pltpu.SemaphoreType.DMA
        vmem, hbm, smem = (pl.BlockSpec(memory_space=m) for m in (pltpu.VMEM, pltpu.HBM, pltpu.SMEM))
        return pl.pallas_call(
            functools.partial(layers_kernel, (n, layers, tok, width, dec, seq, hd, ff)),
            out_shape=jax.ShapeDtypeStruct((tok, width), BF16),
            in_specs=[smem, vmem, vmem] + [hbm] * 10,
            out_specs=vmem,
            scratch_shapes=[
                pltpu.VMEM((ncol, tok, LANES), BF16),
                pltpu.VMEM((ncol, tok, LANES), BF16),
                pltpu.VMEM((ncol // 2, tok, LANES), BF16),
                pltpu.VMEM((chips, half, LANES), BF16),
                pltpu.VMEM((chips, half, LANES), BF16),
                pltpu.VMEM((tok, width), BF16),
                pltpu.VMEM((tok, 3 * hd), BF16),
                pltpu.VMEM((dec, BLOCK * hd), BF16),
                pltpu.VMEM((dec, seq), F32),
                pltpu.VMEM((dec, seq), BF16),
                pltpu.VMEM((tok, hd), BF16),
                pltpu.VMEM((tok, ff), BF16),
                pltpu.VMEM((tok, LANES), F32),
                pltpu.VMEM((tok, LANES), F32),
                pltpu.VMEM((dec, LANES), jnp.int32),
                pltpu.VMEM((2 * layers, width), F32),
                pltpu.VMEM((layers, 3 * hd, width), BF16),
                pltpu.VMEM((layers, hd, width), BF16),
                pltpu.VMEM((layers, width, ff), BF16),
                pltpu.VMEM((layers, width, ff), BF16),
                pltpu.VMEM((layers, ff, width), BF16),
                pltpu.VMEM((layers, rows * hd, seq), BF16),
                pltpu.VMEM((layers, rows * hd, seq), BF16),
                dma((ncol,)),
                dma((layers, 11)),
                dma((2,)), dma((2,)), dma((2,)), dma((2,)), dma((2,)), dma((2, chips)), dma((2,)), dma((2,)),
            ],
            compiler_params=pltpu.CompilerParams(collective_id=0, has_side_effects=True, vmem_limit_bytes=63 * 2**20),
        )(lengths, attn_gain, mlp_gain, x, turned(w_q), turned(w_k), turned(w_v), w_o, w_gate, w_up, w_down, flat(k_cache), flat(v_cache))

    return jax.shard_map(body, mesh=mesh, in_specs=in_specs, out_specs=P("dp", None), check_vma=False)
```

```python
import functools

import jax
import jax.numpy as jnp
from jax import lax
from jax.experimental import pallas as pl
from jax.experimental.pallas import tpu as pltpu
from jax.sharding import PartitionSpec as P

ROPE_BASE = 500000.0
EPSILON = 1e-5
MESH = pl.DeviceIdType.MESH
LANES = 128
SUBLANES = 8
BLOCK = 16
DECODE_STREAMS, PREFILL_STREAMS = 2, 2
ORDER = (3, 0, 0, 1, 2, 0, 3, 0, 2, 3, 1, 2, 1, 0, 1, 3, 2, 0, 0, 0, 0, 3, 0, 2, 3, 1, 3, 3, 2, 2, 2, 3, 2, 0, 1, 1, 1, 3, 1, 2, 0, 1, 0, 0, 0, 0, 3, 2, 1, 0, 3, 3, 2, 2, 3, 2, 3, 1, 0, 2, 1, 1, 1, 1, 3, 1, 2, 0, 0, 3, 1, 2, 3, 0, 3, 3, 2, 0, 2, 3, 2, 1, 2, 1, 1, 1, 0, 1, 3, 2, 0, 1, 2, 0, 3, 1, 3, 2, 0, 1)
MIB = 2**20
PIECE = MIB // 2
PACE = {"start": 2 * MIB, "middle": 4 * MIB, "end": 2 * MIB, "scatter": MIB // 2, "spread": MIB // 2, "forward": 0, "finish": 0}
F32 = jnp.float32
BF16 = jnp.bfloat16


def nt_dot(a, b):
    return lax.dot_general(a, b, (((1,), (1,)), ((), ())), preferred_element_type=F32)


def split_rows(dec, chunk):
    d, c = dec // DECODE_STREAMS, chunk // PREFILL_STREAMS
    rows = [(i * d, d) for i in range(DECODE_STREAMS)] + [(dec + i * c, c) for i in range(PREFILL_STREAMS)]
    return tuple(rows), DECODE_STREAMS


def stage_order(streams, decode_streams, phases):
    chains = []
    for s in range(len(streams)):
        chain = []
        for phase in range(phases):
            middle = ["middle"] if s < decode_streams and phase % 2 == 0 else []
            chain += [(s, name, phase) for name in ["start"] + middle + ["end", "scatter", "spread", "forward", "finish"]]
        chains.append(iter(chain))
    return [next(chains[s]) for s in ORDER]


def layers_kernel(dims, len_ref, again_ref, mgain_ref, x_hbm, wq_hbm, wk_hbm, wv_hbm, wo_hbm, wg_hbm, wu_hbm, wd_hbm, kc_hbm, vc_hbm, out_ref,
                  hbuf, part, pair_in, mine, rs_in, normed, qkv, qbd, logits, probs, v_self, attended, act, cos_ref, sin_ref, len_col, gains,
                  wqkv, wo, wg, wu, wd, kc, vc,
                  x_sem, w_sem, pair_send, pair_recv, rs_send, rs_recv, ag_send, ag_recv, fwd_send, fwd_recv):
    n, layers, tok, width, dec, seq, hd, ff = dims
    chips = n // 2
    side = int(round(chips ** 0.5))
    chunk = tok - dec
    ncol = width // LANES
    ngrp = ncol // 2
    me = lax.axis_index("tp")
    core = lax.rem(me, 2)
    chip = me // 2
    my_y, my_x = chip // side, lax.rem(chip, side)
    partner = chip * 2 + (1 - core)
    my_base, other_base = core * ngrp, (1 - core) * ngrp
    streams, decode_streams = split_rows(dec, chunk)

    def hops(step):
        return sum(min(d, side - d) for d in divmod(step, side))

    peers = []
    for step in sorted(range(1, chips), key=lambda step: -hops(step)):
        at = lax.rem(my_y + step // side, side) * side + lax.rem(my_x + step % side, side)
        peers.append((at, at * 2 + core, lax.rem(at, ngrp), at // ngrp))

    barrier = pltpu.get_barrier_semaphore()
    pl.semaphore_signal(barrier, inc=1, device_id={"tp": partner}, device_id_type=MESH)

    for _, device, _, _ in peers:
        pl.semaphore_signal(barrier, inc=1, device_id={"tp": device}, device_id_type=MESH)

    def x_copy(c):
        return pltpu.make_async_copy(x_hbm.at[:, pl.ds(c * LANES, LANES)], hbuf.at[c], x_sem.at[c])

    def parts_of(l, name):
        def cache(src, dst, first, rows, i):
            at = pl.ds(first * hd, rows * hd)
            return src.at[l, at], dst.at[l, at], w_sem.at[l, i], rows * hd

        if name[:4] in ("keys", "valu"):
            s = int(name[-1])
            src, dst, i = (kc_hbm, kc, 9 + 2 * s) if name[0] == "k" else (vc_hbm, vc, 10 + 2 * s)
            return cache(src, dst, *streams[s], i)
        return {
            "q": lambda: (wq_hbm.at[l], wqkv.at[l, pl.ds(0, hd)], w_sem.at[l, 0], hd),
            "k": lambda: (wk_hbm.at[l], wqkv.at[l, pl.ds(hd, hd)], w_sem.at[l, 1], hd),
            "v": lambda: (wv_hbm.at[l], wqkv.at[l, pl.ds(2 * hd, hd)], w_sem.at[l, 2], hd),
            "o": lambda: (wo_hbm.at[l], wo.at[l], w_sem.at[l, 3], hd),
            "gate": lambda: (wg_hbm.at[l], wg.at[l], w_sem.at[l, 4], width),
            "up": lambda: (wu_hbm.at[l], wu.at[l], w_sem.at[l, 5], width),
            "down": lambda: (wd_hbm.at[l], wd.at[l], w_sem.at[l, 6], ff),
            "pre_keys": lambda: cache(kc_hbm, kc, dec, 1, 7),
            "pre_values": lambda: cache(vc_hbm, vc, dec, 1, 8),
        }[name]()

    def load(l, name):
        src, dst, sem, _ = parts_of(l, name)
        return pltpu.make_async_copy(src, dst, sem)

    early = ("q", "k", "v", "pre_keys", "pre_values")
    late = [f"{kind}{s}" for s in range(decode_streams) for kind in ("keys", "values")] + ["o", "gate", "up", "down"]
    pending = []
    for l in range(1, layers):
        for name in (*early, "o", *late[:-4], "gate", "up", "down"):
            src, dst, sem, rows = parts_of(l, name)
            piece = min(rows, PIECE // (2 * src.shape[-1]))
            pending += [(src.at[pl.ds(at, piece)], dst.at[pl.ds(at, piece)], sem, piece * src.shape[-1] * 2) for at in range(0, rows, piece)]

    def prefetch(budget):
        while pending and budget > 0:
            src, dst, sem, size = pending.pop(0)
            pltpu.make_async_copy(src, dst, sem).start()
            budget -= size

    for c in range(ncol):
        x_copy(c).start()
    for name in early:
        load(0, name).start()

    row8 = lax.broadcasted_iota(jnp.int32, (SUBLANES, LANES), 0)
    for b in range(dec // SUBLANES):
        col = jnp.zeros((SUBLANES, LANES), jnp.int32)
        for i in range(SUBLANES):
            col = jnp.where(row8 == i, len_ref[b * SUBLANES + i], col)
        len_col[b * SUBLANES:(b + 1) * SUBLANES, :] = col
    prefix = len_ref[dec]
    lane_f = lax.broadcasted_iota(jnp.int32, (1, LANES), 1)
    freq_exps = (2 * lax.rem(lane_f, hd // 2)).astype(F32) / hd
    freqs = jnp.exp(-freq_exps * jnp.log(jnp.full((1, LANES), ROPE_BASE, F32)))
    sign = jnp.where(lax.rem(lane_f, hd) < hd // 2, -1.0, 1.0)
    pos = jnp.concatenate([len_col[...], prefix + lax.broadcasted_iota(jnp.int32, (chunk, LANES), 0)], axis=0)
    angles = pos.astype(F32) * freqs
    cos_ref[...] = jnp.cos(angles)
    sin_ref[...] = jnp.sin(angles) * sign
    for first, ref in ((0, again_ref), (layers, mgain_ref)):
        gain = ref[...].astype(F32)
        for l in range(layers):
            for c in range(ncol):
                gains[first + l, c] = gain[l:l + 1, c * LANES:(c + 1) * LANES]

    for c in range(ncol):
        x_copy(c).wait()
    for name in late:
        load(0, name).start()

    def norm(s, gain_row):
        r0, rows = streams[s]
        h = hbuf[:, r0:r0 + rows, :].astype(F32)
        total = jnp.sum(jnp.sum(h * h, axis=0), axis=1, keepdims=True)
        inv = lax.rsqrt(total / width + EPSILON)
        h = (hbuf[:, r0:r0 + rows, :].astype(F32) * inv[None] * gains[gain_row]).astype(BF16)
        for c in range(ncol):
            normed[r0:r0 + rows, c * LANES:(c + 1) * LANES] = h[c]

    def project_qkv(s, l):
        r0, rows = streams[s]
        proj = nt_dot(normed[r0:r0 + rows, :], wqkv[l]).astype(BF16)
        lane = lax.broadcasted_iota(jnp.int32, (rows, LANES), 1)
        qk = proj[:, :2 * hd].astype(F32)
        turned = jnp.where(lax.rem(lane, hd) < hd // 2, pltpu.roll(qk, LANES - hd // 2, 1), pltpu.roll(qk, hd // 2, 1))
        qk = (qk * cos_ref[r0:r0 + rows, :] + turned * sin_ref[r0:r0 + rows, :]).astype(BF16)
        qkv[r0:r0 + rows, :2 * hd] = qk
        qkv[r0:r0 + rows, 2 * hd:3 * hd] = proj[:, 2 * hd:]

    scale = hd ** -0.5

    def decode_logits(s, l):
        r0, rows = streams[s]
        lane = lax.broadcasted_iota(jnp.int32, (rows, LANES), 1)
        qk = qkv[r0:r0 + rows, :2 * hd].astype(F32)
        swapped = pltpu.roll(qk, hd, 1)
        q_twice = jnp.where(lane < hd, qk, swapped)
        k_twice = jnp.where(lane < hd, swapped, qk)
        row = lax.rem(lax.broadcasted_iota(jnp.int32, (rows, LANES), 0), BLOCK)
        for j in range(BLOCK * hd // LANES):
            qbd[r0:r0 + rows, j * LANES:(j + 1) * LANES] = jnp.where(row == 2 * j + lane // hd, q_twice, 0.0).astype(BF16)
        self_logit = jnp.sum(jnp.where(lane < hd, q_twice * k_twice, 0.0), axis=1, keepdims=True) * scale
        need(l, f"keys{s}")
        span = BLOCK * hd
        for g in range(r0 // BLOCK, (r0 + rows) // BLOCK):
            at = slice(g * BLOCK, (g + 1) * BLOCK)
            logits[at, :] = jnp.dot(qbd[at, :], kc[l, g * span:(g + 1) * span, :], preferred_element_type=F32)
        pos = lax.broadcasted_iota(jnp.int32, (rows, seq), 1)
        lg = jnp.where(pos < len_col[r0:r0 + rows, 0:1], logits[r0:r0 + rows, :] * scale, -jnp.inf)
        top = jnp.maximum(jnp.max(lg, axis=1, keepdims=True), self_logit)
        ex = jnp.exp(lg - top)
        ex_self = jnp.exp(self_logit - top)
        inv = 1.0 / (jnp.sum(ex, axis=1, keepdims=True) + ex_self)
        probs[r0:r0 + rows, :] = (ex * inv).astype(BF16)
        p_self = (ex_self * inv).astype(BF16).astype(F32)
        v_self[r0:r0 + rows, :] = p_self * qkv[r0:r0 + rows, 2 * hd:3 * hd].astype(F32)

    def decode_values(s, l):
        need(l, f"values{s}")
        r0, rows = streams[s]
        span = BLOCK * hd
        lane_b = lax.broadcasted_iota(jnp.int32, (BLOCK, LANES), 1)
        row_b = lax.broadcasted_iota(jnp.int32, (BLOCK, LANES), 0)

        for g in range(r0 // BLOCK, (r0 + rows) // BLOCK):
            at = slice(g * BLOCK, (g + 1) * BLOCK)
            full = nt_dot(probs[at, :], vc[l, g * span:(g + 1) * span, :])
            acc = jnp.zeros((BLOCK, LANES), F32)
            for j in range(BLOCK * hd // LANES):
                acc += jnp.where(row_b == 2 * j + lane_b // hd, full[:, j * LANES:(j + 1) * LANES], 0.0)
            acc += pltpu.roll(acc, hd, 1)
            attended[at, :] = (acc[:, 0:hd] + v_self[at, :]).astype(BF16)

    def prefill_attention(s, l):
        r0, rows = streams[s]
        seen = r0 + rows - dec
        q_chk = qkv[r0:r0 + rows, 0:hd]
        lg = jnp.dot(q_chk, kc[l, dec * hd:(dec + 1) * hd, :], preferred_element_type=F32) * scale
        lg_new = nt_dot(q_chk, qkv[dec:dec + seen, hd:2 * hd]) * scale
        pos = lax.broadcasted_iota(jnp.int32, (rows, seq), 1)
        lg = jnp.where(pos < prefix, lg, -jnp.inf)
        tok_r = lax.broadcasted_iota(jnp.int32, (rows, seen), 0) + (r0 - dec)
        tok_c = lax.broadcasted_iota(jnp.int32, (rows, seen), 1)
        lg_new = jnp.where(tok_c <= tok_r, lg_new, -jnp.inf)
        top = jnp.maximum(jnp.max(lg, axis=1, keepdims=True), jnp.max(lg_new, axis=1, keepdims=True))
        ex, ex_new = jnp.exp(lg - top), jnp.exp(lg_new - top)
        inv = 1.0 / (jnp.sum(ex, axis=1, keepdims=True) + jnp.sum(ex_new, axis=1, keepdims=True))
        p_old = (ex * inv).astype(BF16)
        p_new = (ex_new * inv).astype(BF16)
        out = nt_dot(p_old, vc[l, dec * hd:(dec + 1) * hd, :])
        out += jnp.dot(p_new, qkv[dec:dec + seen, 2 * hd:3 * hd], preferred_element_type=F32)
        attended[r0:r0 + rows, :] = out.astype(BF16)

    def remote(src, dst, send, recv, dev):
        return pltpu.make_async_remote_copy(src_ref=src, dst_ref=dst, send_sem=send, recv_sem=recv, device_id={"tp": dev}, device_id_type=MESH)

    def pair_copy(s):
        r0, rows = streams[s]
        return remote(part.at[pl.ds(other_base, ngrp), pl.ds(r0, rows)], pair_in.at[:, pl.ds(r0, rows)], pair_send.at[s], pair_recv.at[s], partner)

    met = []

    def project_out(s, lhs_ref, w_ref):
        r0, rows = streams[s]
        lhs = lhs_ref[r0:r0 + rows, :]
        step = min(4, ngrp)
        for base in (other_base, my_base):
            for c in range(0, ngrp, step):
                at = pl.multiple_of((base + c) * LANES, LANES)
                out = jnp.dot(lhs, w_ref[:, pl.ds(at, step * LANES)], preferred_element_type=F32).astype(BF16)
                for j in range(step):
                    part[base + c + j, r0:r0 + rows, :] = out[:, j * LANES:(j + 1) * LANES]
            if base is other_base:
                if not met:
                    met.append(True)
                    pl.semaphore_wait(barrier, chips)
                pair_copy(s).start()

    def block_at(s, group, half):
        r0, rows = streams[s]
        return group, pl.ds(pl.multiple_of(r0 + half * (rows // 2), rows // 2), rows // 2)

    own_group, own_half = lax.rem(chip, ngrp), chip // ngrp
    targets = [[block_at(s, group, half) for _, _, group, half in peers] for s in range(len(streams))]

    def own_rows(s):
        r0, rows = streams[s]
        return pl.ds(r0 // 2, rows // 2)

    loaded = set()

    def need(l, *names):
        for name in names:
            if (l, name) not in loaded:
                loaded.add((l, name))
                if l > 0 and name not in ("q", "k", "v"):
                    prefetch(1 << 40)
                load(l, name).wait()

    def start_compute(s, phase):
        l = phase // 2
        r0, rows = streams[s]
        norm(s, l + layers * (phase % 2))
        if phase % 2 == 0:
            need(l, "q", "k", "v")
            project_qkv(s, l)
        else:
            need(l, "gate", "up")
            a = normed[r0:r0 + rows, :]
            gate = jnp.dot(a, wg[l], preferred_element_type=F32)
            up = jnp.dot(a, wu[l], preferred_element_type=F32)
            act[r0:r0 + rows, :] = (gate * lax.logistic(gate) * up).astype(BF16)

    def end_compute(s, phase):
        l = phase // 2
        if phase % 2 == 0:
            if s >= decode_streams:
                need(l, "pre_keys", "pre_values")
                prefill_attention(s, l)
            else:
                decode_values(s, l)
            need(l, "o")
            project_out(s, attended, wo.at[l])
        else:
            need(l, "down")
            project_out(s, act, wd.at[l])

    def scatter(s):
        r0, rows = streams[s]
        pair_copy(s).wait()
        both = part[pl.ds(my_base, ngrp), r0:r0 + rows, :].astype(F32) + pair_in[:, r0:r0 + rows, :].astype(F32)
        mine[:, r0:r0 + rows, :] = both.astype(BF16)
        slot = own_rows(s)

        for (_, device, _, _), block in zip(peers, targets[s]):
            remote(mine.at[block], rs_in.at[chip, slot], rs_send.at[s], rs_recv.at[s], device).start()
        rs_in[chip, slot, :] = mine[(*block_at(s, own_group, own_half), slice(None))]

    def peer_blocks(s, send, recv):
        blocks = rs_in.at[pl.ds(0, chips - 1), own_rows(s)]
        return remote(blocks, blocks, send.at[s], recv.at[s], partner)

    def spread(s):
        group, rows = block_at(s, own_group, own_half)
        own = hbuf.at[my_base + group, rows]
        peer_blocks(s, rs_send, rs_recv).wait_recv()
        total = jnp.sum(rs_in[:, own_rows(s), :].astype(F32), axis=0) + hbuf[my_base + group, rows, :].astype(F32)
        hbuf[my_base + group, rows, :] = total.astype(BF16)
        for _, device, _, _ in peers:
            remote(own, own, ag_send.at[s], ag_recv.at[s], device).start()

    def hand_on(s):
        r0, rows = streams[s]
        blocks = hbuf.at[pl.ds(my_base, ngrp), pl.ds(r0, rows)]
        return remote(blocks, blocks, fwd_send.at[s], fwd_recv.at[s], partner)

    def forward(s):
        peer_blocks(s, ag_send, ag_recv).wait_recv()
        hand_on(s).start()

    def finish(s):
        peer_blocks(s, rs_send, rs_recv).wait_send()
        peer_blocks(s, ag_send, ag_recv).wait_send()
        hand_on(s).wait()

    phases = 2 * layers
    stages = {"start": start_compute, "middle": lambda s, phase: decode_logits(s, phase // 2), "end": end_compute, "scatter": lambda s, _: scatter(s), "spread": lambda s, _: spread(s),
              "forward": lambda s, _: forward(s), "finish": lambda s, _: finish(s)}
    order = stage_order(streams, decode_streams, phases)
    settled = max(i for i, (s, name, phase) in enumerate(order) if s < decode_streams and name == "end" and phase == 0)
    for i, (s, name, phase) in enumerate(order):
        if i > settled:
            prefetch(PACE[name])
        stages[name](s, phase)
        if name == "finish" and phase == phases - 1:
            r0, rows = streams[s]

            for c in range(ncol):
                out_ref[r0:r0 + rows, c * LANES:(c + 1) * LANES] = hbuf[c, r0:r0 + rows, :]


def solution(mesh):
    col_spec = P(None, None, "tp")
    row_spec = P(None, "tp", None)
    cache_spec = P(None, "dp", "tp", None, None)
    in_specs = (P("dp", None), P("dp"), P(), col_spec, col_spec, col_spec, row_spec, P(), col_spec, col_spec, row_spec, cache_spec, cache_spec)
    n = mesh.shape["tp"]

    def body(x, lengths, attn_gain, w_q, w_k, w_v, w_o, mlp_gain, w_gate, w_up, w_down, k_cache, v_cache):
        tok, width = x.shape
        layers, rows, _, seq, hd = k_cache.shape
        dec, ff, chips = rows - 1, w_gate.shape[-1], n // 2
        half, ncol, count = tok // 2, width // LANES, DECODE_STREAMS + PREFILL_STREAMS

        def flat(cache):
            return jnp.swapaxes(cache, 3, 4).reshape(layers, rows * hd, seq)

        def turned(w):
            return jnp.swapaxes(w, 1, 2)

        dma = pltpu.SemaphoreType.DMA
        vmem, hbm, smem = (pl.BlockSpec(memory_space=m) for m in (pltpu.VMEM, pltpu.HBM, pltpu.SMEM))
        return pl.pallas_call(
            functools.partial(layers_kernel, (n, layers, tok, width, dec, seq, hd, ff)),
            out_shape=jax.ShapeDtypeStruct((tok, width), BF16),
            in_specs=[smem, vmem, vmem] + [hbm] * 10,
            out_specs=vmem,
            scratch_shapes=[
                pltpu.VMEM((ncol, tok, LANES), BF16),
                pltpu.VMEM((ncol, tok, LANES), BF16),
                pltpu.VMEM((ncol // 2, tok, LANES), BF16),
                pltpu.VMEM((ncol // 2, tok, LANES), BF16),
                pltpu.VMEM((chips, half, LANES), BF16),
                pltpu.VMEM((tok, width), BF16),
                pltpu.VMEM((tok, 3 * hd), BF16),
                pltpu.VMEM((dec, BLOCK * hd), BF16),
                pltpu.VMEM((dec, seq), F32),
                pltpu.VMEM((dec, seq), BF16),
                pltpu.VMEM((dec, hd), F32),
                pltpu.VMEM((tok, hd), BF16),
                pltpu.VMEM((tok, ff), BF16),
                pltpu.VMEM((tok, LANES), F32),
                pltpu.VMEM((tok, LANES), F32),
                pltpu.VMEM((dec, LANES), jnp.int32),
                pltpu.VMEM((2 * layers, ncol, 1, LANES), F32),
                pltpu.VMEM((layers, 3 * hd, width), BF16),
                pltpu.VMEM((layers, hd, width), BF16),
                pltpu.VMEM((layers, width, ff), BF16),
                pltpu.VMEM((layers, width, ff), BF16),
                pltpu.VMEM((layers, ff, width), BF16),
                pltpu.VMEM((layers, rows * hd, seq), BF16),
                pltpu.VMEM((layers, rows * hd, seq), BF16),
                dma((ncol,)),
                dma((layers, 9 + 2 * DECODE_STREAMS)),
                dma((count,)), dma((count,)), dma((count,)), dma((count,)), dma((count,)), dma((count,)), dma((count,)), dma((count,)),
            ],
            compiler_params=pltpu.CompilerParams(collective_id=0, has_side_effects=True, vmem_limit_bytes=63 * 2**20),
        )(lengths, attn_gain, mlp_gain, x, turned(w_q), turned(w_k), turned(w_v), w_o, w_gate, w_up, w_down, flat(k_cache), flat(v_cache))

    return jax.shard_map(body, mesh=mesh, in_specs=in_specs, out_specs=P("dp", None), check_vma=False)
```

```python
import functools

import jax
import jax.numpy as jnp
from jax import lax
from jax.experimental import pallas as pl
from jax.experimental.pallas import tpu as pltpu
from jax.sharding import PartitionSpec as P

ROPE_BASE = 500000.0
EPSILON = 1e-5
MESH = pl.DeviceIdType.MESH
LANES = 128
SUBLANES = 8
BLOCK = 16
DECODE_STREAMS, PREFILL_STREAMS = 2, 2
ORDER = (1, 2, 0, 0, 3, 0, 2, 0, 3, 2, 1, 3, 1, 0, 1, 2, 3, 0, 1, 0, 0, 2, 0, 3, 0, 2, 2, 2, 3, 3, 1, 3, 2, 3, 1, 1, 0, 1, 1, 2, 3, 0, 1, 0, 0, 0, 2, 0, 3, 2, 2, 2, 1, 3, 3, 3, 0, 2, 1, 1, 3, 1, 1, 0, 1, 2, 3, 1, 0, 2, 3, 0, 0, 0, 2, 2, 2, 3, 1, 3, 3, 2, 0, 1, 1, 1, 3, 1, 2, 0, 3, 1, 0, 2, 3, 0, 1, 2, 3, 1)
MIB = 2**20
PIECE = MIB // 2
PACE = {"start": 2 * MIB, "middle": 4 * MIB, "end": MIB, "scatter": 0, "spread": 0, "forward": 0, "finish": 0}
F32 = jnp.float32
BF16 = jnp.bfloat16


def nt_dot(a, b):
    return lax.dot_general(a, b, (((1,), (1,)), ((), ())), preferred_element_type=F32)


def split_rows(dec, chunk):
    d, c = dec // DECODE_STREAMS, chunk // PREFILL_STREAMS
    rows = [(i * d, d) for i in range(DECODE_STREAMS)] + [(dec + i * c, c) for i in range(PREFILL_STREAMS)]
    return tuple(rows), DECODE_STREAMS


def stage_order(streams, decode_streams, phases):
    chains = []
    for s in range(len(streams)):
        chain = []
        for phase in range(phases):
            middle = ["middle"] if s < decode_streams and phase % 2 == 0 else []
            chain += [(s, name, phase) for name in ["start"] + middle + ["end", "scatter", "spread", "forward", "finish"]]
        chains.append(iter(chain))
    return [next(chains[s]) for s in ORDER]


def layers_kernel(dims, len_ref, again_ref, mgain_ref, x_hbm, wq_hbm, wk_hbm, wv_hbm, wo_hbm, wg_hbm, wu_hbm, wd_hbm, kc_hbm, vc_hbm, out_ref,
                  hbuf, part, pair_in, mine, rs_in, normed, qkv, qbd, logits, probs, v_self, attended, act, cos_ref, sin_ref, len_col, gains,
                  wqkv, wo, wg, wu, wd, kc, vc,
                  x_sem, w_sem, pair_send, pair_recv, rs_send, rs_recv, ag_send, ag_recv, fwd_send, fwd_recv, out_sem):
    n, layers, tok, width, dec, seq, hd, ff = dims
    chips = n // 2
    side = int(round(chips ** 0.5))
    chunk = tok - dec
    ncol = width // LANES
    ngrp = ncol // 2
    me = lax.axis_index("tp")
    core = lax.rem(me, 2)
    chip = me // 2
    my_y, my_x = chip // side, lax.rem(chip, side)
    partner = chip * 2 + (1 - core)
    my_base, other_base = core * ngrp, (1 - core) * ngrp
    streams, decode_streams = split_rows(dec, chunk)

    def hops(step):
        return sum(min(d, side - d) for d in divmod(step, side))

    peers = []
    for step in sorted(range(1, chips), key=lambda step: -hops(step)):
        at = lax.rem(my_y + step // side, side) * side + lax.rem(my_x + step % side, side)
        peers.append((at, at * 2 + core, lax.rem(at, ngrp), at // ngrp))

    barrier = pltpu.get_barrier_semaphore()
    pl.semaphore_signal(barrier, inc=1, device_id={"tp": partner}, device_id_type=MESH)

    for _, device, _, _ in peers:
        pl.semaphore_signal(barrier, inc=1, device_id={"tp": device}, device_id_type=MESH)

    def x_copy(c):
        return pltpu.make_async_copy(x_hbm.at[:, pl.ds(c * LANES, LANES)], hbuf.at[c], x_sem.at[c])

    def parts_of(l, name):
        def cache(src, dst, first, rows, i):
            at = pl.ds(first * hd, rows * hd)
            return src.at[l, at], dst.at[l, at], w_sem.at[l, i], rows * hd

        if name[:4] in ("keys", "valu"):
            s = int(name[-1])
            src, dst, i = (kc_hbm, kc, 9 + 2 * s) if name[0] == "k" else (vc_hbm, vc, 10 + 2 * s)
            return cache(src, dst, *streams[s], i)
        return {
            "q": lambda: (wq_hbm.at[l], wqkv.at[l, pl.ds(0, hd)], w_sem.at[l, 0], hd),
            "k": lambda: (wk_hbm.at[l], wqkv.at[l, pl.ds(hd, hd)], w_sem.at[l, 1], hd),
            "v": lambda: (wv_hbm.at[l], wqkv.at[l, pl.ds(2 * hd, hd)], w_sem.at[l, 2], hd),
            "o": lambda: (wo_hbm.at[l], wo.at[l], w_sem.at[l, 3], hd),
            "gate": lambda: (wg_hbm.at[l], wg.at[l], w_sem.at[l, 4], width),
            "up": lambda: (wu_hbm.at[l], wu.at[l], w_sem.at[l, 5], width),
            "down": lambda: (wd_hbm.at[l], wd.at[l], w_sem.at[l, 6], ff),
            "pre_keys": lambda: cache(kc_hbm, kc, dec, 1, 7),
            "pre_values": lambda: cache(vc_hbm, vc, dec, 1, 8),
        }[name]()

    def load(l, name):
        src, dst, sem, _ = parts_of(l, name)
        return pltpu.make_async_copy(src, dst, sem)

    early = ("q", "k", "v", "pre_keys", "pre_values")
    late = [f"{kind}{s}" for s in range(decode_streams) for kind in ("keys", "values")] + ["o", "gate", "up", "down"]
    pending = []
    for l in range(1, layers):
        for name in (*early, "o", *late[:-4], "gate", "up", "down"):
            src, dst, sem, rows = parts_of(l, name)
            piece = min(rows, PIECE // (2 * src.shape[-1]))
            pending += [(src.at[pl.ds(at, piece)], dst.at[pl.ds(at, piece)], sem, piece * src.shape[-1] * 2) for at in range(0, rows, piece)]

    def prefetch(budget):
        while pending and budget > 0:
            src, dst, sem, size = pending.pop(0)
            pltpu.make_async_copy(src, dst, sem).start()
            budget -= size

    for c in range(ncol):
        x_copy(c).start()
    for name in early:
        load(0, name).start()

    row8 = lax.broadcasted_iota(jnp.int32, (SUBLANES, LANES), 0)
    for b in range(dec // SUBLANES):
        col = jnp.zeros((SUBLANES, LANES), jnp.int32)
        for i in range(SUBLANES):
            col = jnp.where(row8 == i, len_ref[b * SUBLANES + i], col)
        len_col[b * SUBLANES:(b + 1) * SUBLANES, :] = col
    prefix = len_ref[dec]
    lane_f = lax.broadcasted_iota(jnp.int32, (1, LANES), 1)
    freq_exps = (2 * lax.rem(lane_f, hd // 2)).astype(F32) / hd
    freqs = jnp.exp(-freq_exps * jnp.log(jnp.full((1, LANES), ROPE_BASE, F32)))
    sign = jnp.where(lax.rem(lane_f, hd) < hd // 2, -1.0, 1.0)
    pos = jnp.concatenate([len_col[...], prefix + lax.broadcasted_iota(jnp.int32, (chunk, LANES), 0)], axis=0)
    angles = pos.astype(F32) * freqs
    cos_ref[...] = jnp.cos(angles)
    sin_ref[...] = jnp.sin(angles) * sign
    for first, ref in ((0, again_ref), (layers, mgain_ref)):
        gain = ref[...].astype(F32)
        for l in range(layers):
            for c in range(ncol):
                gains[first + l, c] = gain[l:l + 1, c * LANES:(c + 1) * LANES]

    for c in range(ncol):
        x_copy(c).wait()
    for name in late:
        load(0, name).start()

    def norm(s, gain_row):
        r0, rows = streams[s]
        h = hbuf[:, r0:r0 + rows, :].astype(F32)
        total = jnp.sum(jnp.sum(h * h, axis=0), axis=1, keepdims=True)
        inv = lax.rsqrt(total / width + EPSILON)
        h = (hbuf[:, r0:r0 + rows, :].astype(F32) * inv[None] * gains[gain_row]).astype(BF16)
        for c in range(ncol):
            normed[r0:r0 + rows, c * LANES:(c + 1) * LANES] = h[c]

    def project_qkv(s, l):
        r0, rows = streams[s]
        proj = nt_dot(normed[r0:r0 + rows, :], wqkv[l]).astype(BF16)
        lane = lax.broadcasted_iota(jnp.int32, (rows, LANES), 1)
        qk = proj[:, :2 * hd].astype(F32)
        turned = jnp.where(lax.rem(lane, hd) < hd // 2, pltpu.roll(qk, LANES - hd // 2, 1), pltpu.roll(qk, hd // 2, 1))
        qk = (qk * cos_ref[r0:r0 + rows, :] + turned * sin_ref[r0:r0 + rows, :]).astype(BF16)
        qkv[r0:r0 + rows, :2 * hd] = qk
        qkv[r0:r0 + rows, 2 * hd:3 * hd] = proj[:, 2 * hd:]

    scale = hd ** -0.5

    def decode_logits(s, l):
        r0, rows = streams[s]
        lane = lax.broadcasted_iota(jnp.int32, (rows, LANES), 1)
        qk = qkv[r0:r0 + rows, :2 * hd].astype(F32)
        swapped = pltpu.roll(qk, hd, 1)
        q_twice = jnp.where(lane < hd, qk, swapped)
        k_twice = jnp.where(lane < hd, swapped, qk)
        row = lax.rem(lax.broadcasted_iota(jnp.int32, (rows, LANES), 0), BLOCK)
        for j in range(BLOCK * hd // LANES):
            qbd[r0:r0 + rows, j * LANES:(j + 1) * LANES] = jnp.where(row == 2 * j + lane // hd, q_twice, 0.0).astype(BF16)
        self_logit = jnp.sum(jnp.where(lane < hd, q_twice * k_twice, 0.0), axis=1, keepdims=True) * scale
        need(l, f"keys{s}")
        span = BLOCK * hd
        for g in range(r0 // BLOCK, (r0 + rows) // BLOCK):
            at = slice(g * BLOCK, (g + 1) * BLOCK)
            logits[at, :] = jnp.dot(qbd[at, :], kc[l, g * span:(g + 1) * span, :], preferred_element_type=F32)
        pos = lax.broadcasted_iota(jnp.int32, (rows, seq), 1)
        lg = jnp.where(pos < len_col[r0:r0 + rows, 0:1], logits[r0:r0 + rows, :] * scale, -jnp.inf)
        top = jnp.maximum(jnp.max(lg, axis=1, keepdims=True), self_logit)
        ex = jnp.exp(lg - top)
        ex_self = jnp.exp(self_logit - top)
        inv = 1.0 / (jnp.sum(ex, axis=1, keepdims=True) + ex_self)
        probs[r0:r0 + rows, :] = (ex * inv).astype(BF16)
        p_self = (ex_self * inv).astype(BF16).astype(F32)
        v_self[r0:r0 + rows, :] = p_self * qkv[r0:r0 + rows, 2 * hd:3 * hd].astype(F32)

    def decode_values(s, l):
        need(l, f"values{s}")
        r0, rows = streams[s]
        span = BLOCK * hd
        lane_b = lax.broadcasted_iota(jnp.int32, (BLOCK, LANES), 1)
        row_b = lax.broadcasted_iota(jnp.int32, (BLOCK, LANES), 0)

        for g in range(r0 // BLOCK, (r0 + rows) // BLOCK):
            at = slice(g * BLOCK, (g + 1) * BLOCK)
            full = nt_dot(probs[at, :], vc[l, g * span:(g + 1) * span, :])
            acc = jnp.zeros((BLOCK, LANES), F32)
            for j in range(BLOCK * hd // LANES):
                acc += jnp.where(row_b == 2 * j + lane_b // hd, full[:, j * LANES:(j + 1) * LANES], 0.0)
            acc += pltpu.roll(acc, hd, 1)
            attended[at, :] = (acc[:, 0:hd] + v_self[at, :]).astype(BF16)

    def prefill_attention(s, l):
        r0, rows = streams[s]
        seen = r0 + rows - dec
        q_chk = qkv[r0:r0 + rows, 0:hd]
        lg = jnp.dot(q_chk, kc[l, dec * hd:(dec + 1) * hd, :], preferred_element_type=F32) * scale
        lg_new = nt_dot(q_chk, qkv[dec:dec + seen, hd:2 * hd]) * scale
        pos = lax.broadcasted_iota(jnp.int32, (rows, seq), 1)
        lg = jnp.where(pos < prefix, lg, -jnp.inf)
        tok_r = lax.broadcasted_iota(jnp.int32, (rows, seen), 0) + (r0 - dec)
        tok_c = lax.broadcasted_iota(jnp.int32, (rows, seen), 1)
        lg_new = jnp.where(tok_c <= tok_r, lg_new, -jnp.inf)
        top = jnp.maximum(jnp.max(lg, axis=1, keepdims=True), jnp.max(lg_new, axis=1, keepdims=True))
        ex, ex_new = jnp.exp(lg - top), jnp.exp(lg_new - top)
        inv = 1.0 / (jnp.sum(ex, axis=1, keepdims=True) + jnp.sum(ex_new, axis=1, keepdims=True))
        p_old = (ex * inv).astype(BF16)
        p_new = (ex_new * inv).astype(BF16)
        out = nt_dot(p_old, vc[l, dec * hd:(dec + 1) * hd, :])
        out += jnp.dot(p_new, qkv[dec:dec + seen, 2 * hd:3 * hd], preferred_element_type=F32)
        attended[r0:r0 + rows, :] = out.astype(BF16)

    def remote(src, dst, send, recv, dev):
        return pltpu.make_async_remote_copy(src_ref=src, dst_ref=dst, send_sem=send, recv_sem=recv, device_id={"tp": dev}, device_id_type=MESH)

    def pair_copy(s):
        r0, rows = streams[s]
        return remote(part.at[pl.ds(other_base, ngrp), pl.ds(r0, rows)], pair_in.at[:, pl.ds(r0, rows)], pair_send.at[s], pair_recv.at[s], partner)

    met = []

    def project_out(s, lhs_ref, w_ref):
        r0, rows = streams[s]
        lhs = lhs_ref[r0:r0 + rows, :]
        step = min(4, ngrp)
        for base in (other_base, my_base):
            for c in range(0, ngrp, step):
                at = pl.multiple_of((base + c) * LANES, LANES)
                out = jnp.dot(lhs, w_ref[:, pl.ds(at, step * LANES)], preferred_element_type=F32).astype(BF16)
                for j in range(step):
                    part[base + c + j, r0:r0 + rows, :] = out[:, j * LANES:(j + 1) * LANES]
            if base is other_base:
                if not met:
                    met.append(True)
                    pl.semaphore_wait(barrier, chips)
                pair_copy(s).start()

    def block_at(s, group, half):
        r0, rows = streams[s]
        return group, pl.ds(pl.multiple_of(r0 + half * (rows // 2), rows // 2), rows // 2)

    own_group, own_half = lax.rem(chip, ngrp), chip // ngrp
    targets = [[block_at(s, group, half) for _, _, group, half in peers] for s in range(len(streams))]

    def own_rows(s):
        r0, rows = streams[s]
        return pl.ds(r0 // 2, rows // 2)

    loaded = set()

    def need(l, *names):
        for name in names:
            if (l, name) not in loaded:
                loaded.add((l, name))
                if l > 0 and name not in ("q", "k", "v"):
                    prefetch(1 << 40)
                load(l, name).wait()

    def start_compute(s, phase):
        l = phase // 2
        r0, rows = streams[s]
        norm(s, l + layers * (phase % 2))
        if phase % 2 == 0:
            need(l, "q", "k", "v")
            project_qkv(s, l)
        else:
            need(l, "gate", "up")
            a = normed[r0:r0 + rows, :]
            gate = jnp.dot(a, wg[l], preferred_element_type=F32)
            up = jnp.dot(a, wu[l], preferred_element_type=F32)
            act[r0:r0 + rows, :] = (gate * lax.logistic(gate) * up).astype(BF16)

    def end_compute(s, phase):
        l = phase // 2
        if phase % 2 == 0:
            if s >= decode_streams:
                need(l, "pre_keys", "pre_values")
                prefill_attention(s, l)
            else:
                decode_values(s, l)
            need(l, "o")
            project_out(s, attended, wo.at[l])
        else:
            need(l, "down")
            project_out(s, act, wd.at[l])

    def scatter(s):
        r0, rows = streams[s]
        pair_copy(s).wait()
        both = part[pl.ds(my_base, ngrp), r0:r0 + rows, :].astype(F32) + pair_in[:, r0:r0 + rows, :].astype(F32)
        mine[:, r0:r0 + rows, :] = both.astype(BF16)
        slot = own_rows(s)

        for (_, device, _, _), block in zip(peers, targets[s]):
            remote(mine.at[block], rs_in.at[chip, slot], rs_send.at[s], rs_recv.at[s], device).start()
        rs_in[chip, slot, :] = mine[(*block_at(s, own_group, own_half), slice(None))]

    def peer_blocks(s, send, recv):
        blocks = rs_in.at[pl.ds(0, chips - 1), own_rows(s)]
        return remote(blocks, blocks, send.at[s], recv.at[s], partner)

    def spread(s):
        group, rows = block_at(s, own_group, own_half)
        own = hbuf.at[my_base + group, rows]
        peer_blocks(s, rs_send, rs_recv).wait_recv()
        total = jnp.sum(rs_in[:, own_rows(s), :].astype(F32), axis=0) + hbuf[my_base + group, rows, :].astype(F32)
        hbuf[my_base + group, rows, :] = total.astype(BF16)
        for _, device, _, _ in peers:
            remote(own, own, ag_send.at[s], ag_recv.at[s], device).start()

    def hand_on(s):
        r0, rows = streams[s]
        blocks = hbuf.at[pl.ds(my_base, ngrp), pl.ds(r0, rows)]
        return remote(blocks, blocks, fwd_send.at[s], fwd_recv.at[s], partner)

    def forward(s):
        peer_blocks(s, ag_send, ag_recv).wait_recv()
        hand_on(s).start()

    def finish(s):
        peer_blocks(s, rs_send, rs_recv).wait_send()
        peer_blocks(s, ag_send, ag_recv).wait_send()
        hand_on(s).wait()

    phases = 2 * layers
    stages = {"start": start_compute, "middle": lambda s, phase: decode_logits(s, phase // 2), "end": end_compute, "scatter": lambda s, _: scatter(s), "spread": lambda s, _: spread(s),
              "forward": lambda s, _: forward(s), "finish": lambda s, _: finish(s)}
    order = stage_order(streams, decode_streams, phases)
    settled = max(i for i, (s, name, phase) in enumerate(order) if s < decode_streams and name == "end" and phase == 0)
    for i, (s, name, phase) in enumerate(order):
        if i > settled:
            prefetch(PACE[name])
        stages[name](s, phase)
        if name == "finish" and phase == phases - 1:
            r0, rows = streams[s]

            for c in range(ncol):
                pltpu.make_async_copy(hbuf.at[c, pl.ds(r0, rows)], out_ref.at[pl.ds(r0, rows), pl.ds(c * LANES, LANES)], out_sem.at[s]).start()
    for s, (r0, rows) in enumerate(streams):
        pltpu.make_async_copy(normed.at[pl.ds(r0, rows)], out_ref.at[pl.ds(r0, rows)], out_sem.at[s]).wait()


def solution(mesh):
    col_spec = P(None, None, "tp")
    row_spec = P(None, "tp", None)
    cache_spec = P(None, "dp", "tp", None, None)
    in_specs = (P("dp", None), P("dp"), P(), col_spec, col_spec, col_spec, row_spec, P(), col_spec, col_spec, row_spec, cache_spec, cache_spec)
    n = mesh.shape["tp"]

    def body(x, lengths, attn_gain, w_q, w_k, w_v, w_o, mlp_gain, w_gate, w_up, w_down, k_cache, v_cache):
        tok, width = x.shape
        layers, rows, _, seq, hd = k_cache.shape
        dec, ff, chips = rows - 1, w_gate.shape[-1], n // 2
        half, ncol, count = tok // 2, width // LANES, DECODE_STREAMS + PREFILL_STREAMS

        def flat(cache):
            return jnp.swapaxes(cache, 3, 4).reshape(layers, rows * hd, seq)

        def turned(w):
            return jnp.swapaxes(w, 1, 2)

        dma = pltpu.SemaphoreType.DMA
        vmem, hbm, smem = (pl.BlockSpec(memory_space=m) for m in (pltpu.VMEM, pltpu.HBM, pltpu.SMEM))
        return pl.pallas_call(
            functools.partial(layers_kernel, (n, layers, tok, width, dec, seq, hd, ff)),
            out_shape=jax.ShapeDtypeStruct((tok, width), BF16),
            in_specs=[smem, vmem, vmem] + [hbm] * 10,
            out_specs=hbm,
            scratch_shapes=[
                pltpu.VMEM((ncol, tok, LANES), BF16),
                pltpu.VMEM((ncol, tok, LANES), BF16),
                pltpu.VMEM((ncol // 2, tok, LANES), BF16),
                pltpu.VMEM((ncol // 2, tok, LANES), BF16),
                pltpu.VMEM((chips, half, LANES), BF16),
                pltpu.VMEM((tok, width), BF16),
                pltpu.VMEM((tok, 3 * hd), BF16),
                pltpu.VMEM((dec, BLOCK * hd), BF16),
                pltpu.VMEM((dec, seq), F32),
                pltpu.VMEM((dec, seq), BF16),
                pltpu.VMEM((dec, hd), F32),
                pltpu.VMEM((tok, hd), BF16),
                pltpu.VMEM((tok, ff), BF16),
                pltpu.VMEM((tok, LANES), F32),
                pltpu.VMEM((tok, LANES), F32),
                pltpu.VMEM((dec, LANES), jnp.int32),
                pltpu.VMEM((2 * layers, ncol, 1, LANES), F32),
                pltpu.VMEM((layers, 3 * hd, width), BF16),
                pltpu.VMEM((layers, hd, width), BF16),
                pltpu.VMEM((layers, width, ff), BF16),
                pltpu.VMEM((layers, width, ff), BF16),
                pltpu.VMEM((layers, ff, width), BF16),
                pltpu.VMEM((layers, rows * hd, seq), BF16),
                pltpu.VMEM((layers, rows * hd, seq), BF16),
                dma((ncol,)),
                dma((layers, 9 + 2 * DECODE_STREAMS)),
                *[dma((count,)) for _ in range(9)],
            ],
            compiler_params=pltpu.CompilerParams(collective_id=0, has_side_effects=True, vmem_limit_bytes=63 * 2**20),
        )(lengths, attn_gain, mlp_gain, x, turned(w_q), turned(w_k), turned(w_v), w_o, w_gate, w_up, w_down, flat(k_cache), flat(v_cache))

    return jax.shard_map(body, mesh=mesh, in_specs=in_specs, out_specs=P("dp", None), check_vma=False)
```
